256 devices in a mesh: lat: 32 (over x_lo, z, core), wid: 8 (over x_hi, y).
Axes of the slice: x: 4 (x_hi: 2, x_lo: 2; x = x_hi * 2 + x_lo), y: 4, z: 8, core: 2. Of those that a mesh axis runs over, the one named last changes fastest.
Arguments:
- buffer_src: bfloat16 [1728, 3584], P('lat', 'wid'), may hold values from -6 to 6
- buffer_tgt: bfloat16 [1728, 3, 3584], P('lat', None, 'wid'), may hold values from -6 to 6
- batch_rows: int32 [1536], replicated, may hold values from 0 to 1727, as said below
- enc_w: float32 [3584, 8192], P('wid', 'lat'), may hold values from -0.09375 to 0.09375
- enc_b: float32 [8192], P('lat'), may hold values from -3 to 3
- dec_w: float32 [3, 8192, 3584], P(None, 'lat', 'wid'), may hold values from -0.0625 to 0.0625
- dec_b: float32 [3, 3584], P(None, 'wid'), may hold values from -3 to 3
- enc_m: float32 [3584, 8192], P('wid', 'lat'), may hold values from -40 to 40
- enc_v: float32 [3584, 8192], P('wid', 'lat'), may hold values from 3 to 300
- dec_m: float32 [3, 8192, 3584], P(None, 'lat', 'wid'), may hold values from -20 to 20
- dec_v: float32 [3, 8192, 3584], P(None, 'lat', 'wid'), may hold values from 3 to 300
Outputs:
- enc_w_new: float32 [3584, 8192], P('wid', 'lat')
- enc_m_new: float32 [3584, 8192], P('wid', 'lat')
- enc_v_new: float32 [3584, 8192], P('wid', 'lat')
- dec_w_new: float32 [3, 8192, 3584], P(None, 'lat', 'wid')
- dec_m_new: float32 [3, 8192, 3584], P(None, 'lat', 'wid')
- dec_v_new: float32 [3, 8192, 3584], P(None, 'lat', 'wid')
The draws below stay inside these ranges and needn't reach their ends.
Inputs may be any that keep to these rules, and one draw needn't show every extreme that they name: `batch_rows`: 1536 different rows of the buffer.
All inputs are finite; a program needn't handle non-finite values.
Results may differ from the reference program's by a relative error of at most 0.0035.
Values may be sent and summed in bfloat16 or wider, within the bound.
No kernel may reach another device: no remote copies, remote signals or barrier semaphores. Data moves between devices by JAX's collectives and lax.ppermute only.
A program may use at most 128 MiB of HBM per device.

```python
import math
import jax
import jax.numpy as jnp

D = 3584
LATENTS = 8192
TARGETS = 3
STEP = 100
TOK = 1536
BUFFER = 1728


def draw_batch_rows(key, part):
    return jax.random.permutation(key, BUFFER)[:TOK].astype(jnp.int32)


def level_of(rng, extent, split, low, high):
    loudness = 1.0
    for dim, blocks in split:
        steps = jax.random.uniform(jax.random.fold_in(jax.random.fold_in(rng, 6), dim), (blocks,), jnp.float32, low / len(split), high / len(split))
        loudness = loudness * jnp.repeat(jnp.exp(steps), extent[dim] // blocks).reshape((-1,) + (1,) * (len(extent) - 1 - dim))
    return loudness


def centred(stream_key, shape, width, reach, split=(), kind=jnp.bfloat16):
    gain = level_of(stream_key, shape, split, -0.22, 0.18) if split else 1.0
    entries = jax.random.normal(stream_key, shape, jnp.float32) * width * gain
    return jnp.minimum(jnp.maximum(entries, -reach), reach).astype(kind)


def setup_inputs(seed: int = 0) -> dict:
    keys = jax.random.split(jax.random.key(seed), 12)
    return {
        "buffer_src": centred(keys[0], (BUFFER, D), 1.0, 6.0, ((0, 32), (1, 8))),
        "buffer_tgt": centred(keys[1], (BUFFER, TARGETS, D), 1.0, 6.0, ((0, 32), (2, 8))),
        "batch_rows": draw_batch_rows(jax.random.fold_in(keys[11], 71), 0),
        "enc_w": centred(keys[3], (D, LATENTS), D ** -0.5, 0.09375, ((0, 8), (1, 32)), jnp.float32),
        "enc_b": centred(keys[4], (LATENTS,), 0.5, 3.0, ((0, 32),), jnp.float32),
        "dec_w": centred(keys[5], (TARGETS, LATENTS, D), LATENTS ** -0.5, 0.0625, ((1, 32), (2, 8)), jnp.float32),
        "dec_b": centred(keys[6], (TARGETS, D), 0.5, 3.0, ((1, 8),), jnp.float32),
        "enc_m": centred(keys[7], (D, LATENTS), 10.0, 40.0, ((0, 8), (1, 32)), jnp.float32),
        "enc_v": jnp.clip(jnp.exp(math.log(300.0) - 4.6051702 * jax.random.uniform(keys[8], (D, LATENTS), jnp.float32) ** level_of(keys[8], (D, LATENTS), ((0, 8), (1, 32)), -0.2, 0.2)), 3.0, 300.0),
        "dec_m": centred(keys[9], (TARGETS, LATENTS, D), 5.0, 20.0, ((1, 32), (2, 8)), jnp.float32),
        "dec_v": jnp.clip(jnp.exp(math.log(300.0) - 4.6051702 * jax.random.uniform(keys[10], (TARGETS, LATENTS, D), jnp.float32) ** level_of(keys[10], (TARGETS, LATENTS, D), ((1, 32), (2, 8)), -0.2, 0.2)), 3.0, 300.0),
    }


def smooth(pre):
    return jax.nn.softplus(4.0 * pre) * 0.25

def adam(weight, grad, first, second):
    first_new = 0.9 * first + 0.1 * grad
    second_new = 0.999 * second + 0.001 * grad * grad
    fix_one = 1.0 - 0.9 ** STEP
    fix_two = 1.0 - 0.999 ** STEP
    weight_new = weight - 0.001 * (first_new / fix_one) / (jnp.sqrt(second_new / fix_two) + 1e-08)
    return (weight_new, first_new, second_new)

def reference(buffer_src, buffer_tgt, batch_rows, enc_w, enc_b, dec_w, dec_b, enc_m, enc_v, dec_m, dec_v):
    source = buffer_src[batch_rows]
    target = buffer_tgt[batch_rows]
    enc_half = enc_w.astype(jnp.bfloat16)
    dec_half = dec_w.astype(jnp.bfloat16)
    pre = jnp.dot(source, enc_half, preferred_element_type=jnp.float32) + enc_b
    act = smooth(pre).astype(jnp.bfloat16)
    slope = jax.nn.sigmoid(4.0 * pre)
    grads = []
    grad_act = jnp.zeros(pre.shape, jnp.float32)
    for layer in range(TARGETS):
        pred = jnp.dot(act, dec_half[layer], preferred_element_type=jnp.float32) + dec_b[layer]
        err = (pred - target[:, layer].astype(jnp.float32)).astype(jnp.bfloat16)
        grads.append(jnp.dot(act.T, err, preferred_element_type=jnp.float32))
        grad_act = grad_act + jnp.dot(err, dec_half[layer].T, preferred_element_type=jnp.float32)
    grad_dec = jnp.stack(grads, 0)
    grad_pre = (grad_act * slope).astype(jnp.bfloat16)
    grad_enc = jnp.dot(source.T, grad_pre, preferred_element_type=jnp.float32)
    enc_w_new, enc_m_new, enc_v_new = adam(enc_w, grad_enc, enc_m, enc_v)
    dec_w_new, dec_m_new, dec_v_new = adam(dec_w, grad_dec, dec_m, dec_v)
    return (enc_w_new, enc_m_new, enc_v_new, dec_w_new, dec_m_new, dec_v_new)
```

```python
import jax
import jax.numpy as jnp
from jax import lax
from jax.sharding import Mesh
from jax.sharding import PartitionSpec as P

STEP = 100
LAT = ("xl", "z", "core")
WID = ("xh", "y")


def swap(block, axis):
    return lax.ppermute(block, axis, [(0, 1), (1, 0)])


def after(block, other):
    return lax.optimization_barrier((block, other))[0]


def collect(shard, axis):
    size = lax.axis_size(axis)
    every = lax.all_to_all(jnp.broadcast_to(shard[None], (size, *shard.shape)), axis, 0, 0, tiled=True)
    return every.reshape(size * shard.shape[0], *shard.shape[1:])


def summed(partial, axis):
    size = lax.axis_size(axis)
    blocks = partial.astype(jnp.bfloat16).reshape(size, partial.shape[0] // size, partial.shape[1])
    blocks = lax.all_to_all(blocks, axis, 0, 0, tiled=True)
    return jnp.sum(blocks.astype(jnp.float32), axis=0)


def matmul(one, two, dims):
    return lax.dot_general(one, two, (dims, ((), ())), preferred_element_type=jnp.float32)


def adam(weight, grad, first, second):
    first_new = 0.9 * first + 0.1 * grad
    second_new = 0.999 * second + 0.001 * grad * grad
    fix_one = 1.0 - 0.9**STEP
    fix_two = 1.0 - 0.999**STEP
    weight_new = weight - 0.001 * (first_new / fix_one) / (jnp.sqrt(second_new / fix_two) + 1e-08)
    return (weight_new, first_new, second_new)


def on_device(
    buffer_src, buffer_tgt, batch_rows, enc_w, enc_b, dec_w, dec_b, enc_m, enc_v, dec_m, dec_v
):
    rows, width = buffer_src.shape
    targets = dec_w.shape[0]
    lats = enc_w.shape[1]
    padded = -(-rows // 8) * 8

    group_src = collect(jnp.pad(buffer_src, ((0, padded - rows), (0, 0))), "z")

    def four(block, axis, cut=None):
        block = jnp.concatenate([block, swap(block, "xl")], axis=axis)
        return jnp.concatenate([block, swap(block, "core")], axis=axis)

    enc_half = four(enc_w.astype(jnp.bfloat16), 1)
    bias = four(enc_b[None], 1)
    dec_own = jnp.concatenate([dec_w[k].astype(jnp.bfloat16) for k in range(targets)], axis=1)
    dec_half = four(after(dec_own, enc_half), 0)

    pre = summed(matmul(group_src, enc_half, ((1,), (0,))), WID) + bias
    act_own = (jax.nn.softplus(4.0 * pre) * 0.25).astype(jnp.bfloat16)
    slope = jax.nn.sigmoid(4.0 * pre)
    act = collect(act_own, WID)

    pred = summed(matmul(act, dec_half, ((1,), (0,))), "z")
    wanted = lax.axis_index(LAT) * rows + lax.iota(jnp.int32, rows)
    used = jnp.any(wanted[:, None] == batch_rows[None, :], axis=1)
    used = jnp.pad(used, (0, padded - rows))
    target = jnp.concatenate([buffer_tgt[:, k] for k in range(targets)], axis=1)
    target = jnp.pad(target, ((0, padded - rows), (0, 0))).astype(jnp.float32)
    shift = dec_b.reshape(1, targets * width)
    err_own = jnp.where(used[:, None], pred + shift - target, 0.0).astype(jnp.bfloat16)
    err = collect(err_own, "z")

    back = summed(matmul(err, dec_half, ((1,), (1,))), WID)

    def four_groups(block):
        blocks = [block, swap(block, "xl")]
        blocks += [swap(one, "core") for one in blocks]
        return blocks

    sources = four_groups(after(group_src, act))

    grad_all = matmul(act, err, ((0,), (0,))).reshape(2, 2, lats, targets * width)
    grad_pair = grad_all[0] + swap(grad_all[1].astype(jnp.bfloat16), "core").astype(jnp.float32)
    grad_dec = grad_pair[0] + swap(grad_pair[1].astype(jnp.bfloat16), "xl").astype(jnp.float32)
    grad_dec = jnp.stack([grad_dec[:, k * width : (k + 1) * width] for k in range(targets)], 0)

    grad_pre = (back * slope).astype(jnp.bfloat16)
    mine, side, core, both = [grad_pre[:, k * lats : (k + 1) * lats] for k in range(4)]
    pieces = [mine, swap(side, "xl"), swap(core, "core"), swap(swap(both, "core"), "xl")]
    grads = collect(jnp.concatenate(pieces, 0)[None], WID)
    size = grads.shape[0]
    grads = grads.reshape(size * 4 * padded, lats)
    source = jnp.stack([one.reshape(size, padded, width) for one in sources], 1)
    source = source.reshape(size * 4 * padded, width)
    grad_enc = matmul(source, grads, ((0,), (0,)))

    dec_w_new, dec_m_new, dec_v_new = adam(dec_w, grad_dec, dec_m, dec_v)
    enc_w_new, enc_m_new, enc_v_new = adam(enc_w, grad_enc, enc_m, enc_v)
    return (enc_w_new, enc_m_new, enc_v_new, dec_w_new, dec_m_new, dec_v_new)


def solution(mesh):
    torus = Mesh(mesh.devices.reshape(2, 8, 2, 2, 4), ("xl", "z", "core", "xh", "y"))
    placed = (
        P(LAT, WID),
        P(LAT, None, WID),
        P(),
        P(WID, LAT),
        P(LAT),
        P(None, LAT, WID),
        P(None, WID),
        P(WID, LAT),
        P(WID, LAT),
        P(None, LAT, WID),
        P(None, LAT, WID),
    )
    return jax.shard_map(
        on_device,
        mesh=torus,
        in_specs=placed,
        out_specs=(
            P(WID, LAT),
            P(WID, LAT),
            P(WID, LAT),
            P(None, LAT, WID),
            P(None, LAT, WID),
            P(None, LAT, WID),
        ),
        check_vma=False,
    )
```

```python
import jax
import jax.numpy as jnp
from jax import lax
from jax.sharding import Mesh
from jax.sharding import PartitionSpec as P

STEP = 100
LAT = ("xl", "zh", "zl", "core")
WID = ("xh", "y")


def swap(block, axis):
    return lax.ppermute(block, axis, [(0, 1), (1, 0)])


def after(block, other):
    return lax.optimization_barrier((block, other))[0]


def collect(shard, axis):
    size = lax.axis_size(axis)
    every = lax.all_to_all(jnp.broadcast_to(shard[None], (size, *shard.shape)), axis, 0, 0, tiled=True)
    return every.reshape(size * shard.shape[0], *shard.shape[1:])


def summed(blocks, axis):
    blocks = lax.all_to_all(blocks.astype(jnp.bfloat16), axis, 0, 0, tiled=True)
    return jnp.sum(blocks.astype(jnp.float32), axis=0)


def in_blocks(partial):
    tokens, lats = partial.shape
    return partial.astype(jnp.bfloat16).reshape(tokens, 8, lats // 8).swapaxes(0, 1)


def to_owner(block):
    axes = ("xl", "zl", "core", *WID)
    pairs = []
    for place in range(64):
        mask = place % 8
        flip = (mask & 1) << 5 | (mask >> 1 & 1) << 4 | (mask >> 2) << 3
        pairs.append((place, place ^ flip))
    return lax.ppermute(block, axes, pairs)


def matmul(one, two, dims):
    return lax.dot_general(one, two, (dims, ((), ())), preferred_element_type=jnp.float32)


def adam(weight, grad, first, second):
    first_new = 0.9 * first + 0.1 * grad
    second_new = 0.999 * second + 0.001 * grad * grad
    fix_one = 1.0 - 0.9**STEP
    fix_two = 1.0 - 0.999**STEP
    weight_new = weight - 0.001 * (first_new / fix_one) / (jnp.sqrt(second_new / fix_two) + 1e-08)
    return (weight_new, first_new, second_new)


def on_device(
    buffer_src, buffer_tgt, batch_rows, enc_w, enc_b, dec_w, dec_b, enc_m, enc_v, dec_m, dec_v
):
    rows, width = buffer_src.shape
    targets, lats = dec_w.shape[:2]
    feats = targets * width
    half = lats // 2
    padded = -(-rows // 8) * 8

    group_src = collect(jnp.pad(buffer_src, ((0, padded - rows), (0, 0))), "zh")
    tokens = group_src.shape[0]

    def eight(block):
        one, two = block[:, :half], block[:, half:]
        one_x = swap(one, "xl")
        two_z = swap(two, "zl")
        one_z = swap(jnp.stack([one, one_x]), "zl")
        two_x = swap(jnp.stack([two, two_z]), "xl")
        parts = [one, two, one_x, two_x[0], one_z[0], two_z, one_z[1], two_x[1]]
        four = jnp.concatenate(parts, axis=1)
        return jnp.concatenate([four, swap(four, "core")], axis=1)

    enc_half = eight(enc_w.astype(jnp.bfloat16))
    dec_own = dec_w.astype(jnp.bfloat16).swapaxes(1, 2).reshape(feats, lats)
    dec_half = eight(after(dec_own, enc_half))
    bias = to_owner(enc_b)

    pre = summed(in_blocks(matmul(group_src, enc_half, ((1,), (0,)))), WID) + bias[None]
    act_own = (jax.nn.softplus(4.0 * pre) * 0.25).astype(jnp.bfloat16)
    slope = jax.nn.sigmoid(4.0 * pre)
    side_src = swap(group_src, "zl")
    act_own, side_src = lax.optimization_barrier((act_own, side_src))
    act = collect(act_own[None], WID).swapaxes(0, 1).reshape(tokens, 8 * lats)

    pred = matmul(act, dec_half, ((1,), (1,))).reshape(-1, padded, feats)
    pred = summed(pred, "zh")
    wanted = lax.axis_index(LAT) * rows + lax.iota(jnp.int32, rows)
    used = jnp.any(wanted[:, None] == batch_rows[None, :], axis=1)
    used = jnp.pad(used, (0, padded - rows))
    target = jnp.concatenate([buffer_tgt[:, k] for k in range(targets)], axis=1)
    target = jnp.pad(target, ((0, padded - rows), (0, 0))).astype(jnp.float32)
    shift = dec_b.reshape(1, feats)
    err_own = jnp.where(used[:, None], pred + shift - target, 0.0).astype(jnp.bfloat16)

    two_src = jnp.stack([group_src, side_src])
    far_src = swap(after(two_src, act), "xl")
    err_own, far_src = lax.optimization_barrier((err_own, far_src))
    four_src = jnp.stack([two_src[0], far_src[0], two_src[1], far_src[1]])
    source = jnp.concatenate([four_src, swap(four_src, "core")]).reshape(8 * tokens, width)

    err = collect(err_own, "zh")

    back = summed(in_blocks(matmul(err, dec_half, ((1,), (0,)))), WID)

    sent = matmul(err, act[:, 4 * lats :], ((0,), (0,))).astype(jnp.bfloat16)
    kept = matmul(err, act[:, : 4 * lats], ((0,), (0,)))
    total = kept + swap(sent, "core").astype(jnp.float32)

    def part(mask, side):
        start = mask * lats + side * half
        return total[:, start : start + half]

    narrow = lambda block: block.astype(jnp.bfloat16)
    wide = lambda block: block.astype(jnp.float32)
    one_send = narrow(jnp.stack([part(2, 0), part(3, 0)]))
    two_send = narrow(jnp.stack([part(1, 1), part(3, 1)]))
    grad_pre, one_send, two_send = lax.optimization_barrier((narrow(back * slope), one_send, two_send))
    one = wide(swap(one_send, "zl"))
    two = wide(swap(two_send, "xl"))
    one = part(0, 0) + one[0] + wide(swap(narrow(part(1, 0) + one[1]), "xl"))
    two = part(0, 1) + two[0] + wide(swap(narrow(part(2, 1) + two[1]), "zl"))
    grad_dec = jnp.concatenate([one, two], axis=1).reshape(targets, width, lats).swapaxes(1, 2)

    grads = collect(to_owner(grad_pre), WID)
    grad_enc = matmul(source, grads, ((0,), (0,)))

    dec_w_new, dec_m_new, dec_v_new = adam(dec_w, grad_dec, dec_m, dec_v)
    enc_w_new, enc_m_new, enc_v_new = adam(enc_w, grad_enc, enc_m, enc_v)
    return (enc_w_new, enc_m_new, enc_v_new, dec_w_new, dec_m_new, dec_v_new)


def solution(mesh):
    torus = Mesh(mesh.devices.reshape(2, 4, 2, 2, 2, 4), (*LAT, *WID))
    placed = (
        P(LAT, WID),
        P(LAT, None, WID),
        P(),
        P(WID, LAT),
        P(LAT),
        P(None, LAT, WID),
        P(None, WID),
        P(WID, LAT),
        P(WID, LAT),
        P(None, LAT, WID),
        P(None, LAT, WID),
    )
    return jax.shard_map(
        on_device,
        mesh=torus,
        in_specs=placed,
        out_specs=(
            P(WID, LAT),
            P(WID, LAT),
            P(WID, LAT),
            P(None, LAT, WID),
            P(None, LAT, WID),
            P(None, LAT, WID),
        ),
        check_vma=False,
    )
```

```python
import jax
import jax.numpy as jnp
from jax import lax
from jax.sharding import Mesh
from jax.sharding import PartitionSpec as P


STEP = 100
LAT = ("xl", "zh", "zl", "core")
WID = ("xh", "y")


def swap(block, axis):
    return lax.ppermute(block, axis, [(0, 1), (1, 0)])


def after(block, other):
    return lax.optimization_barrier((block, other))[0]


def collect(shard, axis):
    size = lax.axis_size(axis)
    every = lax.all_to_all(jnp.broadcast_to(shard[None], (size, *shard.shape)), axis, 0, 0, tiled=True)
    return every.reshape(size * shard.shape[0], *shard.shape[1:])


def together(*values):
    return lax.optimization_barrier(values)


def exchange(blocks, axis):
    return lax.all_to_all(blocks.astype(jnp.bfloat16), axis, 0, 0, tiled=True)


def added(blocks):
    return jnp.sum(blocks.astype(jnp.float32), axis=0)


def in_blocks(partial):
    tokens, lats = partial.shape
    return partial.astype(jnp.bfloat16).reshape(tokens, 8, lats // 8).swapaxes(0, 1)


def to_owner(block):
    axes = ("xl", "zl", "core", *WID)
    pairs = []
    for place in range(64):
        mask = place % 8
        flip = (mask & 1) << 5 | (mask >> 1 & 1) << 4 | (mask >> 2) << 3
        pairs.append((place, place ^ flip))
    return lax.ppermute(block, axes, pairs)


def matmul(one, two, dims):
    return lax.dot_general(one, two, (dims, ((), ())), preferred_element_type=jnp.float32)


def adam(weight, grad, first, second):
    first_new = 0.9 * first + 0.1 * grad
    second_new = 0.999 * second + 0.001 * grad * grad
    fix_one = 1.0 - 0.9**STEP
    fix_two = 1.0 - 0.999**STEP
    weight_new = weight - 0.001 * (first_new / fix_one) / (jnp.sqrt(second_new / fix_two) + 1e-08)
    return (weight_new, first_new, second_new)


def on_device(
    buffer_src, buffer_tgt, batch_rows, enc_w, enc_b, dec_w, dec_b, enc_m, enc_v, dec_m, dec_v
):
    rows, width = buffer_src.shape
    targets, lats = dec_w.shape[:2]
    feats = targets * width
    half = lats // 2
    padded = -(-rows // 8) * 8

    group_src = collect(jnp.pad(buffer_src, ((0, padded - rows), (0, 0))), "zh")
    tokens = group_src.shape[0]

    def eight(block):
        one, two = block[:, :half], block[:, half:]
        one_x, two_z = swap(one, "xl"), swap(two, "zl")

        def finish(one_x, two_z):
            one_pair, two_pair = jnp.stack([one, one_x]), jnp.stack([two, two_z])
            one_z, two_x = swap(one_pair, "zl"), swap(two_pair, "xl")
            parts = [one, two, one_x, two_x[0], one_z[0], two_z, one_z[1], two_x[1]]
            four = jnp.concatenate(parts, axis=1)
            return jnp.concatenate([four, swap(four, "core")], axis=1)

        return one_x, two_z, finish

    one_x, two_z, finish = eight(enc_w.astype(jnp.bfloat16))
    enc_half = finish(one_x, two_z)
    group_src, enc_half = together(group_src, enc_half)
    dec_own = dec_w.astype(jnp.bfloat16).swapaxes(1, 2).reshape(feats, lats)
    one_x, two_z, finish = eight(after(dec_own, enc_half))
    bias = to_owner(enc_b)
    side_src = swap(group_src, "zl")

    blocks = in_blocks(matmul(group_src, enc_half, ((1,), (0,))))
    blocks = exchange(blocks, WID)
    blocks, bias, side_src = together(blocks, bias, side_src)
    pre = added(blocks) + bias[None]
    act_own = (jax.nn.softplus(4.0 * pre) * 0.25).astype(jnp.bfloat16)
    slope = jax.nn.sigmoid(4.0 * pre)
    dec_half = finish(one_x, two_z)
    act = collect(act_own[None], WID)
    act, dec_half = together(act, dec_half)
    act = act.swapaxes(0, 1).reshape(tokens, 8 * lats)

    pred = matmul(act, dec_half, ((1,), (1,))).reshape(-1, padded, feats)
    pred = exchange(pred, "zh")
    two_src = jnp.stack([group_src, side_src])
    far_src = swap(two_src, "xl")
    pred, far_src = together(pred, far_src)
    pred = added(pred)
    wanted = lax.axis_index(LAT) * rows + lax.iota(jnp.int32, rows)
    used = jnp.any(wanted[:, None] == batch_rows[None, :], axis=1)
    used = jnp.pad(used, (0, padded - rows))
    target = jnp.concatenate([buffer_tgt[:, k] for k in range(targets)], axis=1)
    target = jnp.pad(target, ((0, padded - rows), (0, 0))).astype(jnp.float32)
    shift = dec_b.reshape(1, feats)
    err_own = jnp.where(used[:, None], pred + shift - target, 0.0).astype(jnp.bfloat16)

    four_src = jnp.stack([two_src[0], far_src[0], two_src[1], far_src[1]])
    source = jnp.concatenate([four_src, swap(four_src, "core")]).reshape(8 * tokens, width)

    err = collect(err_own, "zh")
    err, source = together(err, source)

    back = exchange(in_blocks(matmul(err, dec_half, ((1,), (0,)))), WID)

    sent = matmul(err, act[:, 4 * lats :], ((0,), (0,))).astype(jnp.bfloat16)
    kept = matmul(err, act[:, : 4 * lats], ((0,), (0,)))
    total = kept + swap(sent, "core").astype(jnp.float32)

    def part(mask, side):
        start = mask * lats + side * half
        return total[:, start : start + half]

    narrow = lambda block: block.astype(jnp.bfloat16)
    wide = lambda block: block.astype(jnp.float32)
    one_send = narrow(jnp.stack([part(2, 0), part(3, 0)]))
    two_send = narrow(jnp.stack([part(1, 1), part(3, 1)]))
    back, one_send, two_send, total = together(back, one_send, two_send, total)
    grad_pre = narrow(added(back) * slope)
    one = wide(swap(one_send, "zl"))
    two = wide(swap(two_send, "xl"))
    one_send, two_send = narrow(part(1, 0) + one[1]), narrow(part(2, 1) + two[1])
    one = part(0, 0) + one[0] + wide(swap(one_send, "xl"))
    two = part(0, 1) + two[0] + wide(swap(two_send, "zl"))
    grad_dec = jnp.concatenate([one, two], axis=1).reshape(targets, width, lats).swapaxes(1, 2)

    grads = to_owner(grad_pre)
    grads = collect(grads, WID)
    grads, dec_new = together(grads, adam(dec_w, grad_dec, dec_m, dec_v))
    grad_enc = matmul(source, grads, ((0,), (0,)))
    enc_w_new, enc_m_new, enc_v_new = adam(enc_w, grad_enc, enc_m, enc_v)
    return (enc_w_new, enc_m_new, enc_v_new, *dec_new)


def solution(mesh):
    torus = Mesh(mesh.devices.reshape(2, 4, 2, 2, 2, 4), (*LAT, *WID))
    placed = (
        P(LAT, WID),
        P(LAT, None, WID),
        P(),
        P(WID, LAT),
        P(LAT),
        P(None, LAT, WID),
        P(None, WID),
        P(WID, LAT),
        P(WID, LAT),
        P(None, LAT, WID),
        P(None, LAT, WID),
    )

    return jax.shard_map(
        on_device,
        mesh=torus,
        in_specs=placed,
        out_specs=(
            P(WID, LAT),
            P(WID, LAT),
            P(WID, LAT),
            P(None, LAT, WID),
            P(None, LAT, WID),
            P(None, LAT, WID),
        ),
        check_vma=False,
    )
```

```python
import jax
import jax.numpy as jnp
from jax import lax
from jax.sharding import Mesh
from jax.sharding import PartitionSpec as P


STEP = 100
LAT = ("xl", "z", "core")
WID = ("xh", "y")


def swap(block, axis):
    return lax.ppermute(block, axis, [(0, 1), (1, 0)])


def after(block, other):
    return lax.optimization_barrier((block, other))[0]


def collect(shard, axis):
    size = lax.axis_size(axis)
    every = lax.all_to_all(jnp.broadcast_to(shard[None], (size, *shard.shape)), axis, 0, 0, tiled=True)
    return every.reshape(size * shard.shape[0], *shard.shape[1:])


def together(*values):
    return lax.optimization_barrier(values)


def narrow(block):
    return block.astype(jnp.bfloat16)


def wide(block):
    return block.astype(jnp.float32)


def exchange(partial, axis):
    size = lax.axis_size(axis)
    blocks = narrow(partial).reshape(size, partial.shape[0] // size, partial.shape[1])
    return lax.all_to_all(blocks, axis, 0, 0, tiled=True)


def added(blocks):
    return jnp.sum(wide(blocks), axis=0)


def matmul(one, two, dims):
    return lax.dot_general(one, two, (dims, ((), ())), preferred_element_type=jnp.float32)


def adam(weight, grad, first, second):
    first_new = 0.9 * first + 0.1 * grad
    second_new = 0.999 * second + 0.001 * grad * grad
    fix_one = 1.0 - 0.9**STEP
    fix_two = 1.0 - 0.999**STEP
    weight_new = weight - 0.001 * (first_new / fix_one) / (jnp.sqrt(second_new / fix_two) + 1e-08)
    return (weight_new, first_new, second_new)


def on_device(
    buffer_src, buffer_tgt, batch_rows, enc_w, enc_b, dec_w, dec_b, enc_m, enc_v, dec_m, dec_v
):
    rows, width = buffer_src.shape
    targets = dec_w.shape[0]
    lats = enc_w.shape[1]
    padded = -(-rows // 8) * 8

    group_src = collect(jnp.pad(buffer_src, ((0, padded - rows), (0, 0))), "z")

    def four(block, axis):
        block = jnp.concatenate([block, swap(block, "xl")], axis=axis)
        return jnp.concatenate([block, swap(block, "core")], axis=axis)

    enc_half = four(enc_w.astype(jnp.bfloat16), 1)
    bias = four(enc_b[None], 1)
    dec_own = narrow(dec_w).swapaxes(1, 2).reshape(targets * width, lats)
    dec_half = four(after(dec_own, enc_half), 1)

    pre = added(exchange(matmul(group_src, enc_half, ((1,), (0,))), WID)) + bias
    act_own = (jax.nn.softplus(4.0 * pre) * 0.25).astype(jnp.bfloat16)
    slope = jax.nn.sigmoid(4.0 * pre)
    act = collect(act_own, WID)

    pred = exchange(matmul(act, dec_half, ((1,), (1,))), "z")
    far_src = swap(after(group_src, act), "xl")
    pred, far_src = together(pred, far_src)
    pred = added(pred)
    wanted = lax.axis_index(LAT) * rows + lax.iota(jnp.int32, rows)
    used = jnp.any(wanted[:, None] == batch_rows[None, :], axis=1)
    used = jnp.pad(used, (0, padded - rows))
    target = jnp.concatenate([buffer_tgt[:, k] for k in range(targets)], axis=1)
    target = jnp.pad(target, ((0, padded - rows), (0, 0))).astype(jnp.float32)
    shift = dec_b.reshape(1, targets * width)
    err_own = jnp.where(used[:, None], pred + shift - target, 0.0).astype(jnp.bfloat16)
    err = collect(err_own, "z")
    pair = jnp.stack([group_src, far_src])
    source = jnp.concatenate([pair, swap(pair, "core")])
    source = source.reshape(4, 8, padded, width).swapaxes(0, 1).reshape(32 * padded, width)
    err, source = together(err, source)

    back = matmul(err, dec_half, ((1,), (0,)))
    back = exchange(back, WID)

    sent = narrow(matmul(err, act[:, 2 * lats :], ((0,), (0,))))
    kept = matmul(err, act[:, : 2 * lats], ((0,), (0,)))
    total = kept + wide(swap(sent, "core"))
    half = lats // 2
    one, two = narrow(total[:, lats : lats + half]), narrow(total[:, lats + half :])
    one = swap(one, "xl")
    two = swap(two, "xl")
    back, one = together(back, one)
    grad_dec = total[:, :lats] + jnp.concatenate([wide(one), wide(two)], axis=1)
    grad_dec = grad_dec.reshape(targets, width, lats).swapaxes(1, 2)
    grad_pre = narrow(added(back) * slope)
    mine, side, core, both = [grad_pre[:, k * lats : (k + 1) * lats] for k in range(4)]
    both = lax.ppermute(both, ("xl", "core"), [(0, 3), (1, 2), (2, 1), (3, 0)])
    pieces = jnp.concatenate([mine, swap(side, "xl"), swap(core, "core"), both], 0)
    grads = collect(pieces, WID)
    grads, dec_new = together(grads, adam(dec_w, grad_dec, dec_m, dec_v))
    grad_enc = matmul(source, grads, ((0,), (0,)))

    enc_w_new, enc_m_new, enc_v_new = adam(enc_w, grad_enc, enc_m, enc_v)
    return (enc_w_new, enc_m_new, enc_v_new, *dec_new)


def solution(mesh):
    torus = Mesh(mesh.devices.reshape(2, 8, 2, 2, 4), ("xl", "z", "core", "xh", "y"))
    placed = (
        P(LAT, WID),
        P(LAT, None, WID),
        P(),
        P(WID, LAT),
        P(LAT),
        P(None, LAT, WID),
        P(None, WID),
        P(WID, LAT),
        P(WID, LAT),
        P(None, LAT, WID),
        P(None, LAT, WID),
    )

    return jax.shard_map(
        on_device,
        mesh=torus,
        in_specs=placed,
        out_specs=(
            P(WID, LAT),
            P(WID, LAT),
            P(WID, LAT),
            P(None, LAT, WID),
            P(None, LAT, WID),
            P(None, LAT, WID),
        ),
        check_vma=False,
    )
```
